64 devices in a mesh: rep: 4 (over x, y), dp: 16 (over z, core).
Axes of the slice: x: 2, y: 2, z: 8, core: 2. Of those that a mesh axis runs over, the one named last changes fastest.
The devices are a block of a 4x4x8 slice.
Arguments:
- x: bfloat16 [64, 4096, 512], P(('rep', 'dp')), parts along dimension 0
- dy: bfloat16 [64, 4096, 512], P(('rep', 'dp')), parts along dimension 0
- w_gate: bfloat16 [2, 512, 1408], P(None, 'dp')
- w_up: bfloat16 [2, 512, 1408], P(None, 'dp')
- w_down: bfloat16 [2, 1408, 512], P(None, 'dp')
Outputs:
- output 1: bfloat16 [64, 4096, 512], P(('rep', 'dp')), parts along dimension 0
- output 2: bfloat16 [8, 512, 1408], P('rep', 'dp'), parts along dimension 0
- output 3: bfloat16 [8, 512, 1408], P('rep', 'dp'), parts along dimension 0
- output 4: bfloat16 [8, 1408, 512], P('rep', 'dp'), parts along dimension 0
There are 4 independent parts. The reference program is written for one: setup_inputs(seed, part) draws one part's arguments, and reference() takes and returns one part's arrays. A program takes and returns all parts, laid end to end along the dimension named above; an argument that names none is the same for every part.
All inputs are finite; a program needn't handle non-finite values.
Results may differ from the reference program's by a relative error of at most 0.018.
Values are sent between devices in bfloat16 or wider.
A program may use at most 768 MiB of HBM per device.

```python
import jax
import jax.numpy as jnp
from jax import lax

SEQUENCES = 16
TOKENS = 4096
D = 512
FF = 1408
LAYERS = 2
NAMES = ("w_gate", "w_up", "w_down")
SHAPES = {"w_gate": (LAYERS, D, FF), "w_up": (LAYERS, D, FF), "w_down": (LAYERS, FF, D)}


def bump(key, n, height):
    away = (jnp.arange(n, dtype=jnp.int32) - jax.random.randint(key, (), 0, n, jnp.int32)) % n
    return jnp.where(away < n // 8, height, 1.0)


def together(key, own, strength):
    shared = jax.random.normal(key, own.shape[1:], jnp.float32)
    return (own + strength * shared) * lax.rsqrt(1 + strength * strength)


def setup_inputs(seed: int = 0, part: int = 0) -> dict:
    kx, kdy, ka, kb, kz, kf, kh, kl, *kw = jax.random.split(jax.random.key(seed), 8 + len(NAMES))
    kx, kdy, ka, kb = (jax.random.fold_in(k, part) for k in (kx, kdy, ka, kb))
    shape = (SEQUENCES, TOKENS, D)
    much_x, much_dy = jax.random.uniform(kz, (2,), jnp.float32, 0.0, 1.0)
    layers = 2.0 ** jax.random.uniform(kl, (LAYERS, 1, 1), jnp.float32, -1.0, 1.0)
    x = together(ka, jax.random.normal(kx, shape, jnp.float32), much_x) * bump(kf, D, 4.0)
    dy = together(kb, jax.random.normal(kdy, shape, jnp.float32), much_dy)
    drawn = {"x": x.astype(jnp.bfloat16), "dy": (dy * (SEQUENCES * TOKENS) ** -0.5).astype(jnp.bfloat16)}
    for key, name in zip(kw, NAMES, strict=True):
        w = jax.random.normal(key, SHAPES[name], jnp.float32) * SHAPES[name][1] ** -0.5
        drawn[name] = (w * {"w_gate": 1.0, "w_up": bump(kh, FF, 4.0), "w_down": layers}[name]).astype(jnp.bfloat16)
    return drawn


def matmul(a, w):
    return jnp.dot(a, w, preferred_element_type=jnp.float32).astype(jnp.bfloat16)


def normed(h):
    wide = h.astype(jnp.float32)
    scale = lax.rsqrt(jnp.mean(wide**2, -1, keepdims=True) + 1e-6)
    return (wide * scale).astype(jnp.bfloat16)


def layer(h, w):
    a = normed(h)
    gate = jnp.dot(a, w["w_gate"], preferred_element_type=jnp.float32)
    up = jnp.dot(a, w["w_up"], preferred_element_type=jnp.float32)
    return h + matmul((jax.nn.silu(gate) * up).astype(jnp.bfloat16), w["w_down"])


def stack(weights, h):
    return lax.scan(lambda h, w: (layer(h, w), None), h, weights)[0]


def reference(x, dy, w_gate, w_up, w_down):
    weights = dict(zip(NAMES, (w_gate, w_up, w_down), strict=True))

    def take(so_far, sequence):
        h, by_y = sequence
        _, back = jax.vjp(stack, weights, h)
        by_weights, by_h = back(by_y)
        return jax.tree.map(lambda total, term: total + term.astype(jnp.float32), so_far, by_weights), by_h

    none_yet = {name: jnp.zeros(w.shape, jnp.float32) for name, w in weights.items()}
    by_weights, by_x = lax.scan(take, none_yet, (x, dy))
    return (by_x, *(by_weights[name].astype(jnp.bfloat16) for name in NAMES))
```

```python
import functools

import jax
import jax.numpy as jnp
from jax import lax
from jax.experimental import pallas as pl
from jax.experimental.pallas import tpu as pltpu
from jax.sharding import PartitionSpec as P

BF16, F32 = jnp.bfloat16, jnp.float32
LANES = 128
TILE = 512
WIDTHS = (4, 4, 3)
EPS = 1e-6


def dot(a, b):
    return jnp.dot(a, b, preferred_element_type=F32)


def dot_nt(a, b):
    return lax.dot_general(a, b, (((1,), (1,)), ((), ())), preferred_element_type=F32)


def dot_tn(a, b):
    return lax.dot_general(a, b, (((0,), (0,)), ((), ())), preferred_element_type=F32)


def blocks(ff):
    start, out = 0, []
    widths = WIDTHS if sum(WIDTHS) * LANES == ff else (1,) * (ff // LANES)
    for w in widths:
        out.append((start, w * LANES))
        start += w * LANES
    return out


def norm(h):
    wide = h.astype(F32)
    scale = lax.rsqrt(jnp.mean(wide * wide, -1, keepdims=True) + EPS)
    return wide, scale, (wide * scale).astype(BF16)


def halves(gu, width):
    n = width // LANES
    gate = jnp.concatenate([gu[:, 2 * i * LANES : (2 * i + 1) * LANES] for i in range(n)], 1)
    up = jnp.concatenate([gu[:, (2 * i + 1) * LANES : (2 * i + 2) * LANES] for i in range(n)], 1)
    return gate, up


def woven(gate, up):
    n = gate.shape[1] // LANES
    parts = []
    for i in range(n):
        parts += [gate[:, i * LANES : (i + 1) * LANES], up[:, i * LANES : (i + 1) * LANES]]
    return jnp.concatenate(parts, 1)


def forward_kernel(x_ref, wgu_ref, wd_ref, h_ref, hid_ref):
    x, _, a = norm(x_ref[...])
    for start, width in blocks(hid_ref.shape[1]):
        gate, up = halves(dot(a, wgu_ref[:, 2 * start : 2 * (start + width)]), width)
        hid_ref[:, start : start + width] = (gate * jax.nn.sigmoid(gate) * up).astype(BF16)
    out = dot(hid_ref[...], wd_ref[...]).astype(BF16)
    h_ref[...] = (x + out.astype(F32)).astype(BF16)


def backward_kernel(h_ref, dy_ref, wgu_ref, wd_ref, dh_ref, dwgu_ref, dwd_ref, hid_ref, dgu_ref, acc_gu, acc_d):
    t = pl.program_id(0)

    @pl.when(t == 0)
    def _():
        acc_gu[...] = jnp.zeros_like(acc_gu)
        acc_d[...] = jnp.zeros_like(acc_d)

    wide, scale, a = norm(h_ref[...])
    dy = dy_ref[...]
    for start, width in blocks(hid_ref.shape[1]):
        gate, up = halves(dot(a, wgu_ref[:, 2 * start : 2 * (start + width)]), width)
        dhid = dot_nt(dy, wd_ref[start : start + width, :]).astype(BF16).astype(F32)
        s = jax.nn.sigmoid(gate)
        act = gate * s
        hid_ref[:, start : start + width] = (act * up).astype(BF16)
        dgate = dhid * up * (s + act * (1.0 - s))
        dup = dhid * act
        dgu_ref[:, 2 * start : 2 * (start + width)] = woven(dgate.astype(BF16), dup.astype(BF16))
    acc_d[...] += dot_tn(hid_ref[...], dy)
    acc_gu[...] += dot_tn(a, dgu_ref[...])
    da = dot_nt(dgu_ref[...], wgu_ref[...]).astype(BF16).astype(F32)
    inner = jnp.mean(da * wide, -1, keepdims=True) * (scale * scale * scale)
    dn = (da * scale - wide * inner).astype(BF16)
    dh_ref[...] = (dy.astype(F32) + dn.astype(F32)).astype(BF16)

    @pl.when(t == pl.num_programs(0) - 1)
    def _():
        dwgu_ref[...] = acc_gu[...].astype(BF16)
        dwd_ref[...] = acc_d[...].astype(BF16)


def params():
    return pltpu.CompilerParams(dimension_semantics=("arbitrary",), vmem_limit_bytes=60 * 2**20)


def once(shape):
    return pl.BlockSpec(shape, lambda t: (0, 0))


def rows(d):
    return pl.BlockSpec((TILE, d), lambda t: (t, 0))


def forward(x, wgu, wd):
    tokens, d = x.shape
    ff = wd.shape[0]
    return pl.pallas_call(
        forward_kernel,
        grid=(tokens // TILE,),
        in_specs=[rows(d), once(wgu.shape), once(wd.shape)],
        out_specs=rows(d),
        out_shape=jax.ShapeDtypeStruct(x.shape, BF16),
        scratch_shapes=[pltpu.VMEM((TILE, ff), BF16)],
        compiler_params=params(),
        cost_estimate=pl.CostEstimate(flops=6 * tokens * d * ff, bytes_accessed=4 * tokens * d, transcendentals=0),
        name="forward",
    )(x, wgu, wd)


def backward(h, dy, wgu, wd):
    tokens, d = h.shape
    ff = wd.shape[0]
    return pl.pallas_call(
        backward_kernel,
        grid=(tokens // TILE,),
        in_specs=[rows(d), rows(d), once(wgu.shape), once(wd.shape)],
        out_specs=[rows(d), once(wgu.shape), once(wd.shape)],
        out_shape=[jax.ShapeDtypeStruct(s, BF16) for s in (h.shape, wgu.shape, wd.shape)],
        scratch_shapes=[
            pltpu.VMEM((TILE, ff), BF16),
            pltpu.VMEM((TILE, 2 * ff), BF16),
            pltpu.VMEM(wgu.shape, F32),
            pltpu.VMEM(wd.shape, F32),
        ],
        compiler_params=params(),
        cost_estimate=pl.CostEstimate(flops=16 * tokens * d * ff, bytes_accessed=6 * tokens * d, transcendentals=0),
        name="backward",
    )(h, dy, wgu, wd)


def weave(gate, up):
    shape = gate.shape
    pair = jnp.stack([t.reshape(*shape[:-1], -1, LANES) for t in (gate, up)], -2)
    return pair.reshape(*shape[:-1], -1)


def unweave(both):
    shape = both.shape
    pair = both.reshape(*shape[:-1], -1, 2, LANES)
    return tuple(pair[..., i, :].reshape(*shape[:-1], -1) for i in range(2))


def solution(mesh):
    def step(x, dy, w_gate, w_up, w_down):
        layers = w_gate.shape[0]
        wgu = weave(w_gate, w_up)
        gathered = [
            tuple(lax.all_gather(w[i], "dp", axis=0, tiled=True) for w in (wgu, w_down)) for i in range(layers)
        ]
        h = [x[0]]
        for i in range(layers - 1):
            h.append(forward(h[-1], *gathered[i]))
        by = dy[0]
        grads = [None] * layers
        for i in reversed(range(layers)):
            by, dwgu, dwd = backward(h[i], by, *gathered[i])
            grads[i] = tuple(lax.psum_scatter(t, "dp", scatter_dimension=0, tiled=True) for t in (dwgu, dwd))
        dgate, dup = unweave(jnp.stack([g[0] for g in grads]))
        return by[None], dgate, dup, jnp.stack([g[1] for g in grads])

    tokens, weight = P(("rep", "dp"), None, None), P(None, "dp", None)
    out = P("rep", "dp", None)
    return jax.shard_map(
        step, mesh=mesh, in_specs=(tokens, tokens, weight, weight, weight), out_specs=(tokens, out, out, out), check_vma=False
    )
```
